32 devices in a mesh: tp: 4 (over z), dp: 8 (over y, x, core).
Axes of the slice: x: 2, y: 2, z: 4, core: 2. Of those that a mesh axis runs over, the one named last changes fastest.
Arguments:
- hidden: bfloat16 [32, 256, 6144], P('dp')
- positions: int32 [256], replicated
- ln1_gain: bfloat16 [6144], replicated
- ln1_bias: bfloat16 [6144], replicated
- w_q: bfloat16 [6144, 6144], P(None, 'tp')
- w_k: bfloat16 [6144, 1024], P(None, 'tp')
- w_v: bfloat16 [6144, 1024], P(None, 'tp')
- w_o: bfloat16 [6144, 6144], P('tp')
- ln2_gain: bfloat16 [6144], replicated
- ln2_bias: bfloat16 [6144], replicated
- w_up: bfloat16 [6144, 24576], P(None, 'tp')
- w_down: bfloat16 [24576, 6144], P('tp')
Outputs:
- output 1: bfloat16 [32, 256, 6144], P('dp')
- output 2: float32 [24576], P('tp')
- output 3: float32 [48], P('tp')
- output 4: float32 [6144], replicated
All inputs are finite; a program needn't handle non-finite values.
Results may differ from the reference program's by a relative error of at most 0.00983148.
Values sent between devices are 32-bit elements.
A program may use at most 1 GiB of HBM per device.

```python
import jax
import jax.numpy as jnp
from jax import lax

D = 6144
HEADS = 48
KV_HEADS = 8
HEAD = 128
FF = 24576
SAMPLES = 32
SEQ_LEN = 256
POS_GAP = 64
ROT_DIM = HEAD // 2
ROPE_BASE = 10000.0
LN_EPS = 1e-5


def setup_inputs(seed: int = 0) -> dict:
    key_list = jax.random.split(jax.random.key(seed), 13)
    sample_shift = jax.random.normal(key_list[0], (SAMPLES, 1, D), jnp.float32)
    token_noise = jax.random.normal(key_list[1], (SAMPLES, SEQ_LEN, D), jnp.float32)
    hidden = (0.8 * sample_shift + 0.6 * token_noise).astype(jnp.bfloat16)
    pos_gaps = jax.random.randint(key_list[2], (SEQ_LEN,), 1, POS_GAP + 1)
    positions = (jnp.cumsum(pos_gaps) - pos_gaps[0]).astype(jnp.int32)

    def normal_weight(key_w, rows_in, cols_out):
        return (jax.random.normal(key_w, (rows_in, cols_out), jnp.float32) * rows_in ** -0.5).astype(jnp.bfloat16)

    def norm_param(key_w):
        return (0.3 * jax.random.normal(key_w, (D,), jnp.float32)).astype(jnp.bfloat16)

    return {
        "hidden": hidden,
        "positions": positions,
        "ln1_gain": norm_param(key_list[3]),
        "ln1_bias": norm_param(key_list[4]),
        "w_q": normal_weight(key_list[5], D, HEADS * HEAD),
        "w_k": normal_weight(key_list[6], D, KV_HEADS * HEAD),
        "w_v": normal_weight(key_list[7], D, KV_HEADS * HEAD),
        "w_o": normal_weight(key_list[8], HEADS * HEAD, D),
        "ln2_gain": norm_param(key_list[9]),
        "ln2_bias": norm_param(key_list[10]),
        "w_up": normal_weight(key_list[11], D, FF),
        "w_down": normal_weight(key_list[12], FF, D),
    }


def layer_norm_1p(in_rows, ln_gain, ln_bias):
    rows_f32 = in_rows.astype(jnp.float32)
    row_mean = jnp.mean(rows_f32, axis=-1, keepdims=True)
    centered = rows_f32 - row_mean
    row_var = jnp.mean(centered * centered, axis=-1, keepdims=True)
    scaled = centered * lax.rsqrt(row_var + LN_EPS)
    return (scaled * (1.0 + ln_gain.astype(jnp.float32)) + ln_bias.astype(jnp.float32)).astype(jnp.bfloat16)


def rope_tables(positions):
    rot_half = ROT_DIM // 2
    inv_freq = ROPE_BASE ** (-2.0 * jnp.arange(rot_half, dtype=jnp.float32) / ROT_DIM)
    pos_angle = positions.astype(jnp.float32)[:, None] * inv_freq[None, :]
    return jnp.cos(pos_angle), jnp.sin(pos_angle)


def apply_rope(heads_in, cos_b, sin_b):
    rot_half = ROT_DIM // 2
    heads_f32 = heads_in.astype(jnp.float32)
    lead_half = heads_f32[..., :rot_half]
    tail_half = heads_f32[..., rot_half:ROT_DIM]
    turned = jnp.concatenate([lead_half * cos_b - tail_half * sin_b, tail_half * cos_b + lead_half * sin_b], axis=-1)
    return jnp.concatenate([turned.astype(jnp.bfloat16), heads_in[..., ROT_DIM:]], axis=-1)


def reference(hidden, positions, ln1_gain, ln1_bias, w_q, w_k, w_v, w_o, ln2_gain, ln2_bias, w_up, w_down):
    q_group = HEADS // KV_HEADS
    cos_t, sin_t = rope_tables(positions)
    cos_b = cos_t[:, None, :]
    sin_b = sin_t[:, None, :]
    causal = jnp.arange(SEQ_LEN)[:, None] >= jnp.arange(SEQ_LEN)[None, :]

    def one_sample(x_rows):
        h_in = layer_norm_1p(x_rows, ln1_gain, ln1_bias)
        q_proj = jnp.dot(h_in, w_q, preferred_element_type=jnp.float32).astype(jnp.bfloat16).reshape(SEQ_LEN, HEADS, HEAD)
        k_proj = jnp.dot(h_in, w_k, preferred_element_type=jnp.float32).astype(jnp.bfloat16).reshape(SEQ_LEN, KV_HEADS, HEAD)
        v_proj = jnp.dot(h_in, w_v, preferred_element_type=jnp.float32).astype(jnp.bfloat16).reshape(SEQ_LEN, KV_HEADS, HEAD)
        q_proj = apply_rope(q_proj, cos_b, sin_b)
        k_proj = apply_rope(k_proj, cos_b, sin_b)
        k_full = jnp.repeat(k_proj, q_group, axis=1)
        v_full = jnp.repeat(v_proj, q_group, axis=1)
        scores = jnp.einsum("qhd,khd->hqk", q_proj.astype(jnp.float32), k_full.astype(jnp.float32)) * HEAD ** -0.5
        scores = jnp.where(causal[None, :, :], scores, -1e30)
        attn_prob = jax.nn.softmax(scores, axis=-1).astype(jnp.bfloat16)
        attn_out = jnp.einsum("hqk,khd->qhd", attn_prob.astype(jnp.float32), v_full.astype(jnp.float32)).astype(jnp.bfloat16)
        head_norm = jnp.sqrt(jnp.sum(jnp.square(attn_out.astype(jnp.float32)), axis=-1))
        o_sum = jnp.dot(attn_out.reshape(SEQ_LEN, HEADS * HEAD), w_o, preferred_element_type=jnp.float32)
        x_mid = (x_rows.astype(jnp.float32) + o_sum).astype(jnp.bfloat16)
        h_mid = layer_norm_1p(x_mid, ln2_gain, ln2_bias)
        mlp_act = jnp.square(jax.nn.relu(jnp.dot(h_mid, w_up, preferred_element_type=jnp.float32)))
        mlp_sum = jnp.dot(mlp_act.astype(jnp.bfloat16), w_down, preferred_element_type=jnp.float32)
        out_rows = (x_mid.astype(jnp.float32) + mlp_sum).astype(jnp.bfloat16)
        sample_means = (
            jnp.mean(mlp_act, axis=0),
            jnp.mean(head_norm, axis=0),
            jnp.mean(h_in.astype(jnp.float32), axis=0),
            jnp.mean(h_mid.astype(jnp.float32), axis=0),
        )
        return out_rows, sample_means

    out_hidden, mean_tuple = lax.map(one_sample, hidden)
    act_mean, head_mean, ln1_mean, ln2_mean = mean_tuple
    f_neuron = jnp.sqrt(jnp.sum(jnp.square(act_mean), axis=0))
    f_head = jnp.sqrt(jnp.sum(jnp.square(head_mean), axis=0))
    f_embed = jnp.sqrt(jnp.sum(jnp.square(ln1_mean), axis=0) + jnp.sum(jnp.square(ln2_mean), axis=0))
    return out_hidden, f_neuron, f_head, f_embed
```

```python
import functools

import jax
import jax.numpy as jnp
from jax import lax
from jax.experimental import pallas as pl
from jax.experimental.pallas import tpu as pltpu
from jax.sharding import PartitionSpec as P

HEAD_DIM = 128
ROT_DIM = 64
ROPE_BASE = 10000.0
LN_EPS = 1e-5
F32 = jnp.float32
BF16 = jnp.bfloat16
MESH_ID = pl.DeviceIdType.MESH

CW = 256
MT = 512
LN_STEPS = 4
WOC = 3
DE = 10
DM = 2
NA = 12
NB = 8
NT = 4
MS_GAP = 24


def rope_tables(positions):
    rot_half = ROT_DIM // 2
    inv_freq = ROPE_BASE ** (-2.0 * jnp.arange(rot_half, dtype=F32) / ROT_DIM)
    pos_angle = positions.astype(F32)[:, None] * inv_freq[None, :]
    cos_t, sin_t = jnp.cos(pos_angle), jnp.sin(pos_angle)
    ones = jnp.ones((positions.shape[0], HEAD_DIM - ROT_DIM), F32)
    cos_full = jnp.concatenate([cos_t, cos_t, ones], axis=1)
    sin_full = jnp.concatenate([-sin_t, sin_t, jnp.zeros_like(ones)], axis=1)
    return cos_full, sin_full


def layer_kernel(dims, x_hbm, cos_ref, sin_ref, g1_ref, b1_ref, g2_ref, b2_ref, wq_hbm, wk_hbm, wv_hbm, wo_hbm, w1_hbm, w2_hbm,
                 y_hbm, p_hbm, on_ref, oh_ref, oe_ref,
                 x_all, h1, h2, act, qk_tmp, k_buf, v_buf, attn, wq_buf, wo_buf, wm_buf,
                 land_a, land_b, pair_sum, total, own_p, stage_o, stage_m,
                 csum1, csum2, nacc, eacc, hacc, stats, stats_in,
                 sem_x, sem_wq, sem_wo, sem_wm, sem_po, sem_pm, sem_own, sem_y,
                 send_a, recv_a, send_b, recv_b, send_st, recv_st):
    n_seq, S, D, FF, QW, KVW, n_dp = dims
    C = D // CW
    K = 2 * n_seq * C
    n_q = QW // KVW
    n_wo = C // WOC
    NPS = LN_STEPS + 2 + n_q + n_wo
    U_Q = LN_STEPS
    U_O = LN_STEPS + 2 + n_q
    G0 = U_O + 1
    n1, n2 = FF // MT, D // MT
    NMS = LN_STEPS + n1 + n2
    MS = C + DE + MS_GAP
    rows = S // LN_STEPS
    group = (QW // HEAD_DIM) // (KVW // HEAD_DIM)
    hpt = KVW // HEAD_DIM
    scale = HEAD_DIM ** -0.5
    LW = D // 8

    z = lax.axis_index("tp")
    me = lax.axis_index("dp")
    is_mid = jnp.logical_or(z == 1, z == 2)
    is_end = jnp.logical_not(is_mid)
    mid_peer = 3 - z
    outer = jnp.where(z == 0, 1, jnp.where(z == 1, 0, jnp.where(z == 2, 3, 2)))

    def x_copy(s):
        return pltpu.make_async_copy(x_hbm.at[s], x_all.at[s], sem_x.at[s])

    def wq_start(i):
        slot = lax.rem(i, 2)

        @pl.when(i == 0)
        def _():
            pltpu.make_async_copy(wk_hbm, wq_buf.at[slot], sem_wq.at[slot]).start()

        @pl.when(i == 1)
        def _():
            pltpu.make_async_copy(wv_hbm, wq_buf.at[slot], sem_wq.at[slot]).start()

        @pl.when(i >= 2)
        def _():
            col = pl.multiple_of((i - 2) * KVW, KVW)
            pltpu.make_async_copy(wq_hbm.at[:, pl.ds(col, KVW)], wq_buf.at[slot], sem_wq.at[slot]).start()

    def wq_wait(i):
        slot = lax.rem(i, 2)
        pltpu.make_async_copy(wk_hbm, wq_buf.at[slot], sem_wq.at[slot]).wait()

    def wo_copy(w):
        slot = lax.rem(w, 2)
        col = pl.multiple_of(w * (WOC * CW), WOC * CW)
        return pltpu.make_async_copy(wo_hbm.at[:, pl.ds(col, WOC * CW)], wo_buf.at[slot], sem_wo.at[slot])

    def wm_start(i):
        slot = lax.rem(i, 2)

        @pl.when(i < n1)
        def _():
            col = pl.multiple_of(i * MT, MT)
            pltpu.make_async_copy(w1_hbm.at[:, pl.ds(col, MT)], wm_buf.at[slot], sem_wm.at[slot]).start()

        @pl.when(i >= n1)
        def _():
            col = pl.multiple_of((i - n1) * MT, MT)
            pltpu.make_async_copy(w2_hbm.at[:, pl.ds(col, MT)], wm_buf.at[slot], sem_wm.at[slot]).start()

    def wm_wait(i):
        slot = lax.rem(i, 2)
        pltpu.make_async_copy(w1_hbm.at[:, pl.ds(0, MT)], wm_buf.at[slot], sem_wm.at[slot]).wait()

    def end_to_mid(k):
        slot = lax.rem(k, NA)
        return pltpu.make_async_remote_copy(
            src_ref=p_hbm.at[k], dst_ref=land_a.at[slot], send_sem=send_a.at[slot], recv_sem=recv_a.at[slot],
            device_id={"tp": outer}, device_id_type=MESH_ID)

    def mid_to_end(k):
        return pltpu.make_async_remote_copy(
            src_ref=total.at[lax.rem(k, NT)], dst_ref=land_a.at[lax.rem(k, NA)], send_sem=send_a.at[lax.rem(k, NT)],
            recv_sem=recv_a.at[lax.rem(k, NA)], device_id={"tp": outer}, device_id_type=MESH_ID)

    def mid_to_mid(k):
        slot = lax.rem(k, NB)
        return pltpu.make_async_remote_copy(
            src_ref=pair_sum.at[slot], dst_ref=land_b.at[slot], send_sem=send_b.at[slot], recv_sem=recv_b.at[slot],
            device_id={"tp": mid_peer}, device_id_type=MESH_ID)

    def own_copy(k):
        slot = lax.rem(k, 2)
        return pltpu.make_async_copy(p_hbm.at[k], own_p.at[slot], sem_own.at[slot])

    def y_copy(k):
        s = lax.rem(lax.div(k, C), n_seq)
        col = pl.multiple_of(lax.rem(k, C) * CW, CW)
        slot = lax.rem(k, 2)
        return pltpu.make_async_copy(x_all.at[s, :, pl.ds(col, CW)], y_hbm.at[s, :, pl.ds(col, CW)], sem_y.at[slot])

    def stats_copy(i):
        peer = lax.rem(me + i, n_dp)
        return pltpu.make_async_remote_copy(
            src_ref=stats, dst_ref=stats_in.at[me], send_sem=send_st.at[i - 1], recv_sem=recv_st.at[me],
            device_id={"dp": peer}, device_id_type=MESH_ID)

    def take_sum(k, value):
        s = lax.rem(lax.div(k, C), n_seq)
        col = pl.multiple_of(lax.rem(k, C) * CW, CW)
        here = x_all.at[s, :, pl.ds(col, CW)]
        here[...] = (here[...].astype(F32) + value).astype(BF16)

    def send_y(k):
        @pl.when(k >= K // 2)
        def _():
            @pl.when(k >= K // 2 + 2)
            def _():
                y_copy(k - 2).wait()
            y_copy(k).start()

    def norm_step(s, step, g_ref, b_ref, dst, csum):
        base = step * rows

        def block(i, carry):
            r0 = pl.multiple_of(base + i * 16, 16)
            v = x_all[s, pl.ds(r0, 16), :].astype(F32)
            mean = jnp.mean(v, axis=-1, keepdims=True)
            cen = v - mean
            var = jnp.mean(cen * cen, axis=-1, keepdims=True)
            out = cen * lax.rsqrt(var + LN_EPS) * (1.0 + g_ref[...].astype(F32)) + b_ref[...].astype(F32)
            dst[pl.ds(r0, 16), :] = out.astype(BF16)
            return carry

        lax.fori_loop(0, rows // 16, block, 0)
        part = jnp.sum(dst[pl.ds(pl.multiple_of(base, rows), rows), :].astype(F32), axis=0, keepdims=True)

        @pl.when(step == 0)
        def _():
            csum[...] = part

        @pl.when(step > 0)
        def _():
            csum[...] += part

        @pl.when(step == LN_STEPS - 1)
        def _():
            mean_c = csum[...] * (1.0 / S)
            eacc[...] += mean_c * mean_c

    lane = lax.broadcasted_iota(jnp.int32, (S, HEAD_DIM), 1)

    def rope(head_bf):
        u = head_bf.astype(F32)
        other = jnp.where(lane < ROT_DIM // 2, pltpu.roll(u, HEAD_DIM - ROT_DIM // 2, 1), pltpu.roll(u, ROT_DIM // 2, 1))
        return (u * cos_ref[...] + other * sin_ref[...]).astype(BF16)

    def attention_step(s, u):
        @pl.when(u == 0)
        def _():
            x_copy(s).wait()

        @pl.when(u < LN_STEPS)
        def _():
            norm_step(s, u, g1_ref, b1_ref, h1, csum1)

        @pl.when(u == LN_STEPS - 2)
        def _():
            @pl.when(s > 0)
            def _():
                wq_start(0)

        @pl.when(jnp.logical_and(u >= U_Q, u < U_O))
        def _():
            i = u - U_Q
            wq_wait(i)

            @pl.when(i + 1 < 2 + n_q)
            def _():
                wq_start(i + 1)

            @pl.when(i == n_q)
            def _():
                wo_copy(0).start()

            r = jnp.dot(h1[...], wq_buf[lax.rem(i, 2)], preferred_element_type=F32)
            qk_tmp[...] = r.astype(BF16)

            @pl.when(i == 0)
            def _():
                for h in range(hpt):
                    k_buf[h] = rope(qk_tmp[:, h * HEAD_DIM:(h + 1) * HEAD_DIM])

            @pl.when(i == 1)
            def _():
                for h in range(hpt):
                    v_buf[h] = qk_tmp[:, h * HEAD_DIM:(h + 1) * HEAD_DIM]

            @pl.when(i >= 2)
            def _():
                qt = i - 2
                kv = lax.div(qt * hpt, group)
                keys = k_buf[kv]
                vals = v_buf[kv]
                row = lax.broadcasted_iota(jnp.int32, (S, S), 0)
                colm = lax.broadcasted_iota(jnp.int32, (S, S), 1)
                causal = row >= colm
                outs = []
                for h in range(hpt):
                    q_h = rope(qk_tmp[:, h * HEAD_DIM:(h + 1) * HEAD_DIM])
                    sc = lax.dot_general(q_h, keys, (((1,), (1,)), ((), ())), preferred_element_type=F32) * scale
                    sc = jnp.where(causal, sc, -1e30)
                    top = jnp.max(sc, axis=-1, keepdims=True)
                    ex = jnp.exp(sc - top)
                    prob = (ex / jnp.sum(ex, axis=-1, keepdims=True)).astype(BF16)
                    outs.append(jnp.dot(prob, vals, preferred_element_type=F32).astype(BF16))
                col = pl.multiple_of(qt * KVW, KVW)
                for h in range(hpt):
                    attn[:, pl.ds(pl.multiple_of(col + h * HEAD_DIM, HEAD_DIM), HEAD_DIM)] = outs[h]
                for h in range(hpt):
                    o_f = attn[:, pl.ds(pl.multiple_of(col + h * HEAD_DIM, HEAD_DIM), HEAD_DIM)].astype(F32)
                    nrm = jnp.sqrt(jnp.sum(o_f * o_f, axis=-1, keepdims=True))
                    mean_n = jnp.sum(nrm, axis=0, keepdims=True) * (1.0 / S)
                    hacc[qt * hpt + h] += jnp.broadcast_to(mean_n * mean_n, (8, HEAD_DIM))

        @pl.when(u >= U_O)
        def _():
            w = u - U_O
            wo_copy(w).wait()

            @pl.when(w + 1 < n_wo)
            def _():
                wo_copy(w + 1).start()

            prod = jnp.dot(attn[...], wo_buf[lax.rem(w, 2)], preferred_element_type=F32)
            for c in range(WOC):
                stage_o[c] = prod[:, c * CW:(c + 1) * CW]
            for c in range(WOC):
                pltpu.make_async_copy(stage_o.at[c], p_hbm.at[C * s + WOC * w + c], sem_po.at[c]).start()

    def attention_step_end(s, u):
        @pl.when(u >= U_O)
        def _():
            for c in range(WOC):
                pltpu.make_async_copy(stage_o.at[c], p_hbm.at[C * s + WOC * (u - U_O) + c], sem_po.at[c]).wait()

    def mlp_step(s, v):
        @pl.when(v < LN_STEPS)
        def _():
            norm_step(s, v, g2_ref, b2_ref, h2, csum2)

        @pl.when(v >= LN_STEPS)
        def _():
            i = v - LN_STEPS
            wm_wait(i)

            @pl.when(i + 1 < n1 + n2)
            def _():
                wm_start(i + 1)

            @pl.when(jnp.logical_and(i + 1 == n1 + n2, s + 1 < n_seq))
            def _():
                wm_start(0)

            @pl.when(i < n1)
            def _():
                up = jnp.dot(h2[...], wm_buf[lax.rem(i, 2)], preferred_element_type=F32)
                up = jnp.maximum(up, 0.0)
                up = up * up
                col = pl.multiple_of(i * MT, MT)
                act[:, pl.ds(col, MT)] = up.astype(BF16)
                mean_n = jnp.sum(up, axis=0, keepdims=True) * (1.0 / S)
                nacc[:, pl.ds(col, MT)] += mean_n * mean_n

            @pl.when(i >= n1)
            def _():
                prod = jnp.dot(act[...], wm_buf[lax.rem(i, 2)], preferred_element_type=F32)
                base = K // 2 + C * s + (MT // CW) * (i - n1)
                for c in range(MT // CW):
                    stage_m[c] = prod[:, c * CW:(c + 1) * CW]
                for c in range(MT // CW):
                    pltpu.make_async_copy(stage_m.at[c], p_hbm.at[base + c], sem_pm.at[c]).start()

    def mlp_step_end(s, v):
        @pl.when(v >= LN_STEPS + n1)
        def _():
            base = K // 2 + C * s + (MT // CW) * (v - LN_STEPS - n1)
            for c in range(MT // CW):
                pltpu.make_async_copy(stage_m.at[c], p_hbm.at[base + c], sem_pm.at[c]).wait()

    def middle_slot(t):
        k = t - DM

        @pl.when(t < K)
        def _():
            @pl.when(t == 0)
            def _():
                own_copy(0).start()

            @pl.when(t + 1 < K)
            def _():
                own_copy(t + 1).start()
            own_copy(t).wait()
            end_to_mid(t).wait_recv()

            @pl.when(t >= NB)
            def _():
                mid_to_mid(t - NB).wait_send()
            pair_sum[lax.rem(t, NB)] = own_p[lax.rem(t, 2)] + land_a[lax.rem(t, NA)]

        @pl.when(jnp.logical_and(k >= 0, k < K))
        def _():
            mid_to_mid(k).wait_recv()

            @pl.when(k >= NT)
            def _():
                mid_to_end(k - NT).wait_send()
            total[lax.rem(k, NT)] = pair_sum[lax.rem(k, NB)] + land_b[lax.rem(k, NB)]

        @pl.when(t < K)
        def _():
            mid_to_mid(t).start()

        @pl.when(jnp.logical_and(k >= 0, k < K))
        def _():
            take_sum(k, total[lax.rem(k, NT)])
            mid_to_end(k).start()
            send_y(k)

    def end_slot(t):
        k = t - DE

        @pl.when(k >= 0)
        def _():
            mid_to_end(k).wait_recv()
            take_sum(k, land_a[lax.rem(k, NA)])
            send_y(k)

        @pl.when(t < K)
        def _():
            @pl.when(t >= NA)
            def _():
                end_to_mid(t - NA).wait_send()
            end_to_mid(t).start()

    x_copy(0).start()
    wq_start(jnp.int32(0))
    for s in range(1, n_seq):
        x_copy(s).start()
    barrier = pltpu.get_barrier_semaphore()
    pl.semaphore_signal(barrier, 1, device_id={"tp": outer}, device_id_type=MESH_ID)

    @pl.when(is_mid)
    def _():
        pl.semaphore_signal(barrier, 1, device_id={"tp": mid_peer}, device_id_type=MESH_ID)
    for i in range(1, n_dp):
        pl.semaphore_signal(barrier, 1, device_id={"dp": lax.rem(me + i, n_dp)}, device_id_type=MESH_ID)

    @pl.when(is_mid)
    def _():
        pl.semaphore_wait(barrier, n_dp + 1)

    @pl.when(is_end)
    def _():
        pl.semaphore_wait(barrier, n_dp)

    nacc[...] = jnp.zeros_like(nacc)
    eacc[...] = jnp.zeros_like(eacc)
    hacc[...] = jnp.zeros_like(hacc)
    stats[...] = jnp.zeros_like(stats)

    def slot(n, carry):
        t = n - G0

        @pl.when(jnp.logical_and(is_mid, t >= 0))
        def _():
            middle_slot(t)

        @pl.when(jnp.logical_and(is_end, t >= 0))
        def _():
            end_slot(t)

        s_a = lax.div(n, NPS)
        u_a = lax.rem(n, NPS)

        @pl.when(n < n_seq * NPS)
        def _():
            attention_step(s_a, u_a)

        @pl.when(t == MS - 2)
        def _():
            wm_start(jnp.int32(0))

        m = jnp.maximum(t - MS, 0)
        s_m = lax.div(m, NMS)
        v_m = lax.rem(m, NMS)
        in_mlp = jnp.logical_and(t >= MS, t < MS + n_seq * NMS)

        @pl.when(in_mlp)
        def _():
            mlp_step(s_m, v_m)

        @pl.when(n < n_seq * NPS)
        def _():
            attention_step_end(s_a, u_a)

        @pl.when(in_mlp)
        def _():
            mlp_step_end(s_m, v_m)

        @pl.when(t == MS + n_seq * NMS)
        def _():
            for r in range(FF // LW):
                stats[r:r + 1, :] = nacc[:, r * LW:(r + 1) * LW]
            for r in range(8):
                stats[8 + r:9 + r, :] = eacc[:, r * LW:(r + 1) * LW]
            per_row = LW // HEAD_DIM
            for h in range(QW // HEAD_DIM):
                stats[16 + h // per_row:17 + h // per_row, (h % per_row) * HEAD_DIM:(h % per_row + 1) * HEAD_DIM] = hacc[h, 0:1, :]

        @pl.when(t == MS + n_seq * NMS + 1)
        def _():
            for i in range(1, n_dp):
                stats_copy(i).start()
        return carry

    lax.fori_loop(0, G0 + K + DE, slot, 0)

    @pl.when(is_mid)
    def _():
        for i in range(NB):
            mid_to_mid(K - NB + i).wait_send()
        for i in range(NT):
            mid_to_end(K - NT + i).wait_send()

    @pl.when(is_end)
    def _():
        for i in range(NA):
            end_to_mid(K - NA + i).wait_send()

    stats_in[me] = stats[...]
    for i in range(1, n_dp):
        peer = lax.rem(me + i, n_dp)
        pltpu.make_async_remote_copy(
            src_ref=stats, dst_ref=stats_in.at[peer], send_sem=send_st.at[i - 1], recv_sem=recv_st.at[peer],
            device_id={"dp": peer}, device_id_type=MESH_ID).wait_recv()
        stats_copy(i).wait_send()
    acc = stats_in[0]
    for i in range(1, n_dp):
        acc = acc + stats_in[i]
    stats[...] = jnp.sqrt(acc)
    for r in range(FF // LW):
        on_ref[:, r * LW:(r + 1) * LW] = stats[r:r + 1, :]
    for r in range(8):
        oe_ref[:, r * LW:(r + 1) * LW] = stats[8 + r:9 + r, :]
    per_row = LW // HEAD_DIM
    for h in range(QW // HEAD_DIM):
        oh_ref[h:h + 1, :] = stats[16 + h // per_row:17 + h // per_row, (h % per_row) * HEAD_DIM:(h % per_row + 1) * HEAD_DIM]
    for i in range(2):
        y_copy(K - 2 + i).wait()


def run_layer(n_dp, hidden, cos_t, sin_t, g1, b1, g2, b2, w_q, w_k, w_v, w_o, w_up, w_down):
    n_seq, S, D = hidden.shape
    QW, KVW, FF = w_q.shape[1], w_k.shape[1], w_up.shape[1]
    C = D // CW
    K = 2 * n_seq * C
    n_q = QW // KVW
    n_heads = QW // HEAD_DIM
    LW = D // 8
    NPS = LN_STEPS + 2 + n_q + C // WOC
    MS = C + DE + MS_GAP
    NMS = LN_STEPS + FF // MT + D // MT
    for s in range(n_seq):
        for j in range(C):
            if s or j >= WOC:
                assert NPS * s + j // WOC - 1 <= C * s + j - 2, "late projection"
            assert MS + NMS * s + LN_STEPS + FF // MT + j // (MT // CW) <= K // 2 + C * s + j - 2, "late product"
        assert MS + NMS * s >= C * (s + 1) + DE, "early MLP"
    assert MS + n_seq * NMS + 2 < K + DE, "late scores"
    assert (QW // KVW) % 1 == 0 and FF == D and C % WOC == 0
    any_spec = pl.BlockSpec(memory_space=pl.ANY)
    vmem_spec = pl.BlockSpec(memory_space=pltpu.VMEM)
    dma = pltpu.SemaphoreType.DMA
    macs = n_seq * S * (D * (QW + 2 * KVW) + QW * D + 2 * D * FF)
    return pl.pallas_call(
        functools.partial(layer_kernel, (n_seq, S, D, FF, QW, KVW, n_dp)),
        out_shape=(
            jax.ShapeDtypeStruct((n_seq, S, D), BF16),
            jax.ShapeDtypeStruct((K, S, CW), F32),
            jax.ShapeDtypeStruct((1, FF), F32),
            jax.ShapeDtypeStruct((n_heads, HEAD_DIM), F32),
            jax.ShapeDtypeStruct((1, D), F32),
        ),
        in_specs=[any_spec] + [vmem_spec] * 6 + [any_spec] * 6,
        out_specs=(any_spec, any_spec, vmem_spec, vmem_spec, vmem_spec),
        scratch_shapes=[
            pltpu.VMEM((n_seq, S, D), BF16),
            pltpu.VMEM((S, D), BF16),
            pltpu.VMEM((S, D), BF16),
            pltpu.VMEM((S, FF), BF16),
            pltpu.VMEM((S, KVW), BF16),
            pltpu.VMEM((KVW // HEAD_DIM, S, HEAD_DIM), BF16),
            pltpu.VMEM((KVW // HEAD_DIM, S, HEAD_DIM), BF16),
            pltpu.VMEM((S, QW), BF16),
            pltpu.VMEM((2, D, KVW), BF16),
            pltpu.VMEM((2, QW, WOC * CW), BF16),
            pltpu.VMEM((2, D, MT), BF16),
            pltpu.VMEM((NA, S, CW), F32),
            pltpu.VMEM((NB, S, CW), F32),
            pltpu.VMEM((NB, S, CW), F32),
            pltpu.VMEM((NT, S, CW), F32),
            pltpu.VMEM((2, S, CW), F32),
            pltpu.VMEM((WOC, S, CW), F32),
            pltpu.VMEM((MT // CW, S, CW), F32),
            pltpu.VMEM((1, D), F32),
            pltpu.VMEM((1, D), F32),
            pltpu.VMEM((1, FF), F32),
            pltpu.VMEM((1, D), F32),
            pltpu.VMEM((n_heads, 8, HEAD_DIM), F32),
            pltpu.VMEM((24, LW), F32),
            pltpu.VMEM((n_dp, 24, LW), F32),
            dma((n_seq,)), dma((2,)), dma((2,)), dma((2,)), dma((WOC,)), dma((MT // CW,)), dma((2,)), dma((2,)),
            dma((NA,)), dma((NA,)), dma((NB,)), dma((NB,)), dma((n_dp - 1,)), dma((n_dp,)),
        ],
        compiler_params=pltpu.CompilerParams(collective_id=0, has_side_effects=True, vmem_limit_bytes=67043328),
        cost_estimate=pl.CostEstimate(flops=2 * macs, bytes_accessed=2 * macs // S, transcendentals=0),
        name="layer",
    )(hidden, cos_t, sin_t, g1, b1, g2, b2, w_q, w_k, w_v, w_o, w_up, w_down)


def solution(mesh):
    n_dp = mesh.shape["dp"]

    def local_layer(hidden, positions, ln1_gain, ln1_bias, w_q, w_k, w_v, w_o, ln2_gain, ln2_bias, w_up, w_down):
        cos_t, sin_t = rope_tables(positions)
        y, _, f_n, f_h, f_e = run_layer(
            n_dp, hidden, cos_t, sin_t, ln1_gain[None], ln1_bias[None], ln2_gain[None], ln2_bias[None],
            w_q, w_k, w_v, w_o, w_up, w_down)
        return y, f_n[0], f_h[:, 0], f_e[0]

    weight_col = P(None, "tp")
    weight_row = P("tp", None)
    return jax.shard_map(
        local_layer,
        mesh=mesh,
        in_specs=(P("dp"), P(), P(), P(), weight_col, weight_col, weight_col, weight_row, P(), P(), weight_col, weight_row),
        out_specs=(P("dp"), P("tp"), P("tp"), P()),
        check_vma=False,
    )
```
